32 devices in a mesh: north: 8 (over y, x, core), deep: 4 (over z).
Axes of the slice: x: 2, y: 2, z: 4, core: 2. Of those that a mesh axis runs over, the one named last changes fastest.
Arguments:
- velocity: float32 [4, 128, 64, 256], P(None, None, 'north', 'deep'), may hold values from -6 to 6
- coupling: float32 [4, 4], replicated, may hold values from -4 to 4
- symbol_x: float32 [128], replicated, may hold values from 0.3 to 3
- symbol_y: float32 [64], replicated, may hold values from 0.3 to 3
- symbol_z: float32 [256], replicated, may hold values from 0.3 to 3
Outputs:
- spectrum: float32 [4, 128, 64, 256], P(None, 'north', 'deep')
The draws below stay inside these ranges and needn't reach their ends.
All inputs are finite; a program needn't handle non-finite values.
Results may differ from the reference program's by a relative error of at most 0.00007.
Values sent between devices are 32-bit elements; how exact they have to be, the bound alone decides.
No kernel may reach another device: no remote copies, remote signals or barrier semaphores. Data moves between devices by JAX's collectives and lax.ppermute only.
A program may use at most 128 MiB of HBM per device.

```python
import jax
import jax.numpy as jnp
from jax import lax

GRID_X = 128
GRID_Y = 64
GRID_Z = 256
FIELDS = 4


def steps_of(rng, dims, pieces, least, top_value):
    loudness = 1.0
    for position, shards_of in pieces:
        steps = jax.random.uniform(jax.random.fold_in(jax.random.fold_in(rng, 6), position), (shards_of,), jnp.float32, least / len(pieces), top_value / len(pieces))
        loudness = loudness * jnp.repeat(jnp.exp(steps), dims[position] // shards_of).reshape((-1,) + (1,) * (len(dims) - 1 - position))
    return loudness


def normal_values(key, shape, deviation, limit, pieces=(), kind=jnp.bfloat16):
    array = jax.random.normal(key, shape, jnp.float32) * deviation
    if len(pieces) > 0:
        array = steps_of(key, shape, pieces, -0.22, 0.18) * array
    return jnp.clip(array, min=-limit, max=limit).astype(kind)


def setup_inputs(seed: int = 0) -> dict:
    key_list = jax.random.split(jax.random.key(seed), 6)
    velocity = normal_values(key_list[0], (FIELDS, GRID_X, GRID_Y, GRID_Z), 1.0, 6.0, ((2, 8), (3, 4)), jnp.float32)
    coupling = normal_values(key_list[1], (FIELDS, FIELDS), 0.7, 4.0, (), jnp.float32)
    symbol_x = jnp.clip(jax.random.uniform(key_list[2], (GRID_X,), jnp.float32, 0.3, 3.0), 0.3, 3.0)
    symbol_y = jnp.clip(jax.random.uniform(key_list[3], (GRID_Y,), jnp.float32, 0.3, 3.0), 0.3, 3.0)
    symbol_z = jnp.clip(jax.random.uniform(key_list[4], (GRID_Z,), jnp.float32, 0.3, 3.0), 0.3, 3.0)
    return dict(velocity=velocity, coupling=coupling, symbol_x=symbol_x, symbol_y=symbol_y, symbol_z=symbol_z)


def basis_table(count):
    rank = jnp.arange(count)
    angle = (jnp.pi / (count + 1)) * (((rank[:, None] + 1) * (rank[None, :] + 1)) % (2 * count + 2)).astype(jnp.float32)
    return jnp.sin(angle) * (2.0 / (count + 1)) ** 0.5


def along_dim(values, dim):
    moved = jnp.tensordot(values, basis_table(values.shape[dim]), axes=([dim], [0]), precision=lax.Precision.HIGHEST)
    return jnp.moveaxis(moved, -1, dim)


def reference(velocity, coupling, symbol_x, symbol_y, symbol_z):
    spectrum = velocity
    spectrum = along_dim(spectrum, 1)
    spectrum = along_dim(spectrum, 2)
    spectrum = along_dim(spectrum, 3)
    symbol = symbol_x[:, None, None] + symbol_y[None, :, None] + symbol_z[None, None, :]
    weight_xyz = 1.0 / (1.0 + symbol)
    mixed_fields = jnp.einsum("ab,bxyz->axyz", coupling, spectrum, precision=lax.Precision.HIGHEST)
    spectrum = weight_xyz * spectrum + (1.0 - weight_xyz) * mixed_fields
    return spectrum
```

```python
import functools

import jax
import jax.numpy as jnp
import numpy as np
from jax import lax
from jax.experimental import pallas as pl
from jax.experimental.pallas import tpu as pltpu
from jax.sharding import PartitionSpec as P

SHARES = (1.0,)


def basis_table(count):
    rank = np.arange(1, count + 1)
    turn = (rank[:, None] * rank[None, :]) % (2 * count + 2)
    return (np.sin(np.pi * turn / (count + 1)) * np.sqrt(2.0 / (count + 1))).astype(np.float32)


def halves(values):
    high = values.astype(jnp.bfloat16)
    low = (values - high.astype(jnp.float32)).astype(jnp.bfloat16)
    return high, low


def product(left, right, dims):
    dot = functools.partial(
        lax.dot_general, dimension_numbers=(dims, ((), ())), preferred_element_type=jnp.float32
    )
    left_high, left_low = left
    right_high, right_low = right
    return dot(left_high, right_high) + (dot(left_high, right_low) + dot(left_low, right_high))


def x_kernel(values_ref, high_ref, low_ref, out_ref):
    fields, lines, depth, count = values_ref.shape
    groups, pieces, rows, width = out_ref.shape
    share = rows // lines
    table = (high_ref[...], low_ref[...])
    for line in range(lines):
        plane = values_ref[:, line].reshape(fields * depth, count)
        modes = product(table, halves(plane), ((1,), (1,)))
        for group in range(groups):
            for piece in range(pieces):
                out_ref[group, piece, pl.ds(line, share, stride=lines), :] = modes[
                    group * share : (group + 1) * share, piece * width : (piece + 1) * width
                ]


def y_kernel(values_ref, high_ref, low_ref, out_ref):
    sources, pieces, rows, width = values_ref.shape
    groups, share, block, _ = out_ref.shape
    lines = rows // share
    table = (high_ref[...], low_ref[...])
    for mode in range(share):
        plane = jnp.concatenate(
            [
                values_ref[:, piece, mode * lines : (mode + 1) * lines, :].reshape(-1, width)
                for piece in range(pieces)
            ],
            axis=1,
        )
        modes = product(table, halves(plane), ((1,), (0,)))
        for group in range(groups):
            out_ref[group, mode] = modes[group * block : (group + 1) * block]


def z_values(values_ref, high_ref, low_ref, fields):
    sources, share, block, lanes = values_ref.shape
    depth = lanes // fields
    table = (high_ref[...], low_ref[...])
    planes = [values_ref[source].reshape(share * block, lanes) for source in range(sources)]
    spectra = []
    for field in range(fields):
        line = jnp.concatenate(
            [plane[:, field * depth : (field + 1) * depth] for plane in planes], axis=1
        )
        spectra.append(product(halves(line), table, ((1,), (0,))))
    return spectra


def z_kernel(first, *refs):
    values_ref, high_ref, low_ref, weight_ref, coupling_ref = refs[:5]
    out_ref, staged, sems = refs[-3:]
    fields = staged.shape[0]
    _, share, block, _ = values_ref.shape
    spectra = z_values(values_ref, high_ref, low_ref, fields)
    weight = weight_ref[...].reshape(share * block, -1)
    copies = []
    for field in range(fields):
        mixed = spectra[0] * coupling_ref[field, 0]
        for other in range(1, fields):
            mixed += spectra[other] * coupling_ref[field, other]
        new = mixed + weight * (spectra[field] - mixed)
        staged[field] = new.reshape(share, block, -1)
        copy = pltpu.make_async_copy(
            staged.at[field], out_ref.at[field, pl.ds(first, share)], sems.at[field]
        )
        copy.start()
        copies.append(copy)
    for copy in copies:
        copy.wait()


def split_table(table):
    table = np.asarray(table, np.float32)
    high = jnp.asarray(table).astype(jnp.bfloat16)
    low = (jnp.asarray(table) - high.astype(jnp.float32)).astype(jnp.bfloat16)
    return high, low


def np_split(table):
    high = table.astype(jnp.bfloat16)
    low = (table - high.astype(np.float32)).astype(jnp.bfloat16)
    return jnp.asarray(high), jnp.asarray(low)


VMEM = pl.BlockSpec(memory_space=pltpu.VMEM)


def cost(flops, moved):
    return pl.CostEstimate(flops=int(flops), bytes_accessed=int(moved), transcendentals=0)


def chunks_of(share):
    bounds, total = [0], 0.0
    for part in SHARES:
        total += part
        bounds.append(round(share * total / sum(SHARES)))
    return [(a, b - a) for a, b in zip(bounds, bounds[1:]) if b > a]


def on_device(north, deep, velocity, coupling, symbol_x, symbol_y, symbol_z):
    fields, count_x, lines, depth = velocity.shape
    count_y, count_z = lines * north, depth * deep
    share_x, share_y = count_x // north, count_y // deep
    lanes = fields * depth
    width = 128 if lanes % 128 == 0 else lanes
    table_x = basis_table(count_x).reshape(north, share_x, count_x)
    high_y, low_y = np_split(basis_table(count_y))
    high_z, low_z = np_split(basis_table(count_z))
    values = jnp.transpose(velocity, (0, 2, 3, 1))
    part_x = lax.dynamic_slice_in_dim(symbol_x, lax.axis_index("north") * share_x, share_x)
    part_y = lax.dynamic_slice_in_dim(symbol_y, lax.axis_index("deep") * share_y, share_y)
    weight = 1.0 / (1.0 + (part_x[:, None, None] + part_y[None, :, None] + symbol_z))
    out = None
    for first, share in chunks_of(share_x):
        high, low = np_split(table_x[:, first : first + share].reshape(north * share, count_x))
        sent = pl.pallas_call(
            x_kernel,
            out_shape=jax.ShapeDtypeStruct((north, lanes // width, share * lines, width), jnp.float32),
            in_specs=[VMEM] * 3,
            out_specs=VMEM,
            cost_estimate=cost(6 * north * share * count_x * lines * lanes, 4 * values.size),
            name="x_modes",
        )(values, high, low)
        lines_here = lax.all_to_all(sent, "north", split_axis=0, concat_axis=0, tiled=True)
        sent = pl.pallas_call(
            y_kernel,
            out_shape=jax.ShapeDtypeStruct((deep, share, share_y, lanes), jnp.float32),
            in_specs=[VMEM] * 3,
            out_specs=VMEM,
            cost_estimate=cost(6 * count_y * count_y * share * lanes, 8 * sent.size),
            name="y_modes",
        )(lines_here, high_y, low_y)
        lines_here = lax.all_to_all(sent, "deep", split_axis=0, concat_axis=0, tiled=True)
        operands = [lines_here, high_z, low_z, weight[first : first + share], coupling]
        specs = [VMEM] * 4 + [pl.BlockSpec(memory_space=pltpu.SMEM)]
        aliases = {}
        if out is not None:
            operands.append(out)
            specs.append(pl.BlockSpec(memory_space=pl.ANY))
            aliases = {5: 0}
        out = pl.pallas_call(
            functools.partial(z_kernel, first),
            out_shape=jax.ShapeDtypeStruct((fields, share_x, share_y, count_z), jnp.float32),
            in_specs=specs,
            out_specs=pl.BlockSpec(memory_space=pl.ANY),
            scratch_shapes=[
                pltpu.VMEM((fields, share, share_y, count_z), jnp.float32),
                pltpu.SemaphoreType.DMA((fields,)),
            ],
            input_output_aliases=aliases,
            cost_estimate=cost(6 * sent.size * count_z, 8 * sent.size),
            name="z_modes",
        )(*operands)
    return out


def solution(mesh):
    placed = (P(None, None, "north", "deep"), P(), P(), P(), P())
    return jax.shard_map(
        functools.partial(on_device, mesh.shape["north"], mesh.shape["deep"]),
        mesh=mesh,
        in_specs=placed,
        out_specs=P(None, "north", "deep", None),
        check_vma=False,
    )
```

```python
import functools

import jax
import jax.numpy as jnp
import numpy as np
from jax import lax
from jax.experimental import pallas as pl
from jax.experimental.pallas import tpu as pltpu
from jax.sharding import PartitionSpec as P

SHARES = (1.0,)


def basis_table(count):
    rank = np.arange(1, count + 1)
    turn = (rank[:, None] * rank[None, :]) % (2 * count + 2)
    return (np.sin(np.pi * turn / (count + 1)) * np.sqrt(2.0 / (count + 1))).astype(np.float32)


def halves(values):
    high = values.astype(jnp.bfloat16)
    low = (values - high.astype(jnp.float32)).astype(jnp.bfloat16)
    return high, low


def product(left, right, dims):
    dot = functools.partial(
        lax.dot_general, dimension_numbers=(dims, ((), ())), preferred_element_type=jnp.float32
    )
    left_high, left_low = left
    right_high, right_low = right
    return dot(left_high, right_high) + (dot(left_high, right_low) + dot(left_low, right_high))


def x_kernel(values_ref, high_ref, low_ref, out_ref):
    fields, lines, depth, count = values_ref.shape
    groups, pieces, rows, width = out_ref.shape
    share = rows // lines
    table = (high_ref[...], low_ref[...])
    for line in range(lines):
        plane = values_ref[:, line].reshape(fields * depth, count)
        modes = product(table, halves(plane), ((1,), (1,)))
        for group in range(groups):
            for piece in range(pieces):
                out_ref[group, piece, pl.ds(line, share, stride=lines), :] = modes[
                    group * share : (group + 1) * share, piece * width : (piece + 1) * width
                ]


def y_kernel(values_ref, high_ref, low_ref, out_ref):
    sources, pieces, rows, width = values_ref.shape
    groups, share, block, _ = out_ref.shape
    lines = rows // share
    table = (high_ref[...], low_ref[...])
    for mode in range(share):
        plane = jnp.concatenate(
            [
                values_ref[:, piece, mode * lines : (mode + 1) * lines, :].reshape(-1, width)
                for piece in range(pieces)
            ],
            axis=1,
        )
        modes = product(table, halves(plane), ((1,), (0,)))
        for group in range(groups):
            out_ref[group, mode] = modes[group * block : (group + 1) * block]


def z_values(values_ref, high_ref, low_ref, fields):
    sources, share, block, lanes = values_ref.shape
    depth = lanes // fields
    table = (high_ref[...], low_ref[...])
    planes = [values_ref[source].reshape(share * block, lanes) for source in range(sources)]
    spectra = []
    for field in range(fields):
        line = jnp.concatenate(
            [plane[:, field * depth : (field + 1) * depth] for plane in planes], axis=1
        )
        spectra.append(product(halves(line), table, ((1,), (0,))))
    return spectra


def z_kernel(first, *refs):
    values_ref, high_ref, low_ref, weight_ref, coupling_ref = refs[:5]
    out_ref, staged, sems = refs[-3:]
    fields = staged.shape[0]
    _, share, block, _ = values_ref.shape
    spectra = z_values(values_ref, high_ref, low_ref, fields)
    weight = weight_ref[...].reshape(share * block, -1)
    copies = []
    for field in range(fields):
        mixed = spectra[0] * coupling_ref[field, 0]
        for other in range(1, fields):
            mixed += spectra[other] * coupling_ref[field, other]
        new = mixed + weight * (spectra[field] - mixed)
        staged[field] = new.reshape(share, block, -1)
        copy = pltpu.make_async_copy(
            staged.at[field], out_ref.at[field, pl.ds(first, share)], sems.at[field]
        )
        copy.start()
        copies.append(copy)
    for copy in copies:
        copy.wait()


def split_table(table):
    table = np.asarray(table, np.float32)
    high = jnp.asarray(table).astype(jnp.bfloat16)
    low = (jnp.asarray(table) - high.astype(jnp.float32)).astype(jnp.bfloat16)
    return high, low


def np_split(table):
    high = table.astype(jnp.bfloat16)
    low = (table - high.astype(np.float32)).astype(jnp.bfloat16)
    return jnp.asarray(high), jnp.asarray(low)


VMEM = pl.BlockSpec(memory_space=pltpu.VMEM)


def cost(flops, moved):
    return pl.CostEstimate(flops=int(flops), bytes_accessed=int(moved), transcendentals=0)


def chunks_of(share):
    bounds, total = [0], 0.0
    for part in SHARES:
        total += part
        bounds.append(round(share * total / sum(SHARES)))
    return [(a, b - a) for a, b in zip(bounds, bounds[1:]) if b > a]


def on_device(north, deep, velocity, coupling, symbol_x, symbol_y, symbol_z):
    fields, count_x, lines, depth = velocity.shape
    count_y, count_z = lines * north, depth * deep
    share_x, share_y = count_x // north, count_y // deep
    lanes = fields * depth
    width = 128 if lanes % 128 == 0 else lanes
    table_x = basis_table(count_x).reshape(north, share_x, count_x)
    high_y, low_y = np_split(basis_table(count_y))
    high_z, low_z = np_split(basis_table(count_z))
    values = jnp.transpose(velocity, (0, 2, 3, 1))
    part_x = lax.dynamic_slice_in_dim(symbol_x, lax.axis_index("north") * share_x, share_x)
    part_y = lax.dynamic_slice_in_dim(symbol_y, lax.axis_index("deep") * share_y, share_y)
    weight = 1.0 / (1.0 + (part_x[:, None, None] + part_y[None, :, None] + symbol_z))
    out = None
    for first, share in chunks_of(share_x):
        high, low = np_split(table_x[:, first : first + share].reshape(north * share, count_x))
        sent = pl.pallas_call(
            x_kernel,
            out_shape=jax.ShapeDtypeStruct((north, lanes // width, share * lines, width), jnp.float32),
            in_specs=[VMEM] * 3,
            out_specs=VMEM,
            compiler_params=pltpu.CompilerParams(vmem_limit_bytes=16 * 2**20),
            cost_estimate=cost(6 * north * share * count_x * lines * lanes, 4 * values.size),
            name="x_modes",
        )(values, high, low)
        lines_here = lax.all_to_all(sent, "north", split_axis=0, concat_axis=0, tiled=True)
        sent = pl.pallas_call(
            y_kernel,
            out_shape=jax.ShapeDtypeStruct((deep, share, share_y, lanes), jnp.float32),
            in_specs=[VMEM] * 3,
            out_specs=VMEM,
            compiler_params=pltpu.CompilerParams(vmem_limit_bytes=16 * 2**20),
            cost_estimate=cost(6 * count_y * count_y * share * lanes, 8 * sent.size),
            name="y_modes",
        )(lines_here, high_y, low_y)
        lines_here = lax.all_to_all(sent, "deep", split_axis=0, concat_axis=0, tiled=True)
        operands = [lines_here, high_z, low_z, weight[first : first + share], coupling]
        specs = [VMEM] * 4 + [pl.BlockSpec(memory_space=pltpu.SMEM)]
        aliases = {}
        if out is not None:
            operands.append(out)
            specs.append(pl.BlockSpec(memory_space=pl.ANY))
            aliases = {5: 0}
        out = pl.pallas_call(
            functools.partial(z_kernel, first),
            out_shape=jax.ShapeDtypeStruct((fields, share_x, share_y, count_z), jnp.float32),
            in_specs=specs,
            out_specs=pl.BlockSpec(memory_space=pl.ANY),
            scratch_shapes=[
                pltpu.VMEM((fields, share, share_y, count_z), jnp.float32),
                pltpu.SemaphoreType.DMA((fields,)),
            ],
            input_output_aliases=aliases,
            compiler_params=pltpu.CompilerParams(vmem_limit_bytes=16 * 2**20),
            cost_estimate=cost(6 * sent.size * count_z, 8 * sent.size),
            name="z_modes",
        )(*operands)
    return out


def solution(mesh):
    placed = (P(None, None, "north", "deep"), P(), P(), P(), P())
    return jax.shard_map(
        functools.partial(on_device, mesh.shape["north"], mesh.shape["deep"]),
        mesh=mesh,
        in_specs=placed,
        out_specs=P(None, "north", "deep", None),
        check_vma=False,
    )
```

```python
import functools

import jax
import jax.numpy as jnp
import numpy as np
from jax import lax
from jax.experimental import pallas as pl
from jax.experimental.pallas import tpu as pltpu
from jax.sharding import PartitionSpec as P

SHARES = (5, 11)


def basis_table(count):
    rank = np.arange(1, count + 1)
    turn = (rank[:, None] * rank[None, :]) % (2 * count + 2)
    return (np.sin(np.pi * turn / (count + 1)) * np.sqrt(2.0 / (count + 1))).astype(np.float32)


def halves(values):
    high = values.astype(jnp.bfloat16)
    low = (values - high.astype(jnp.float32)).astype(jnp.bfloat16)
    return high, low


def product(left, right, dims):
    dot = functools.partial(
        lax.dot_general, dimension_numbers=(dims, ((), ())), preferred_element_type=jnp.float32
    )
    left_high, left_low = left
    right_high, right_low = right
    return dot(left_high, right_high) + (dot(left_high, right_low) + dot(left_low, right_high))


def x_kernel(values_ref, high_ref, low_ref, out_ref):
    fields, lines, depth, count = values_ref.shape
    groups, pieces, rows, width = out_ref.shape
    share = rows // lines
    table = (high_ref[...], low_ref[...])
    for line in range(lines):
        plane = values_ref[:, line].reshape(fields * depth, count)
        modes = product(table, halves(plane), ((1,), (1,)))
        for group in range(groups):
            for piece in range(pieces):
                out_ref[group, piece, pl.ds(line, share, stride=lines), :] = modes[
                    group * share : (group + 1) * share, piece * width : (piece + 1) * width
                ]


def y_kernel(values_ref, high_ref, low_ref, out_ref):
    sources, pieces, rows, width = values_ref.shape
    groups, share, block, _ = out_ref.shape
    lines = rows // share
    table = (high_ref[...], low_ref[...])
    for mode in range(share):
        plane = jnp.concatenate(
            [
                values_ref[:, piece, mode * lines : (mode + 1) * lines, :].reshape(-1, width)
                for piece in range(pieces)
            ],
            axis=1,
        )
        modes = product(table, halves(plane), ((1,), (0,)))
        for group in range(groups):
            out_ref[group, mode] = modes[group * block : (group + 1) * block]


def z_values(values_ref, high_ref, low_ref, fields):
    sources, share, block, lanes = values_ref.shape
    depth = lanes // fields
    table = (high_ref[...], low_ref[...])
    planes = [values_ref[source].reshape(share * block, lanes) for source in range(sources)]
    spectra = []
    for field in range(fields):
        line = jnp.concatenate(
            [plane[:, field * depth : (field + 1) * depth] for plane in planes], axis=1
        )
        spectra.append(product(halves(line), table, ((1,), (0,))))
    return spectra


def z_kernel(first, *refs):
    values_ref, high_ref, low_ref, weight_ref, coupling_ref = refs[:5]
    out_ref, staged, sems = refs[-3:]
    fields = staged.shape[0]
    _, share, block, _ = values_ref.shape
    spectra = z_values(values_ref, high_ref, low_ref, fields)
    weight = weight_ref[...].reshape(share * block, -1)
    copies = []
    for field in range(fields):
        mixed = spectra[0] * coupling_ref[field, 0]
        for other in range(1, fields):
            mixed += spectra[other] * coupling_ref[field, other]
        new = mixed + weight * (spectra[field] - mixed)
        staged[field] = new.reshape(share, block, -1)
        copy = pltpu.make_async_copy(
            staged.at[field], out_ref.at[field, pl.ds(first, share)], sems.at[field]
        )
        copy.start()
        copies.append(copy)
    for copy in copies:
        copy.wait()


def split_table(table):
    table = np.asarray(table, np.float32)
    high = jnp.asarray(table).astype(jnp.bfloat16)
    low = (jnp.asarray(table) - high.astype(jnp.float32)).astype(jnp.bfloat16)
    return high, low


def np_split(table):
    high = table.astype(jnp.bfloat16)
    low = (table - high.astype(np.float32)).astype(jnp.bfloat16)
    return jnp.asarray(high), jnp.asarray(low)


VMEM = pl.BlockSpec(memory_space=pltpu.VMEM)


def cost(flops, moved):
    return pl.CostEstimate(flops=int(flops), bytes_accessed=int(moved), transcendentals=0)


def chunks_of(share):
    bounds, total = [0], 0.0
    for part in SHARES:
        total += part
        bounds.append(round(share * total / sum(SHARES)))
    return [(a, b - a) for a, b in zip(bounds, bounds[1:]) if b > a]


def on_device(north, deep, velocity, coupling, symbol_x, symbol_y, symbol_z):
    fields, count_x, lines, depth = velocity.shape
    count_y, count_z = lines * north, depth * deep
    share_x, share_y = count_x // north, count_y // deep
    lanes = fields * depth
    width = 128 if lanes % 128 == 0 else lanes
    table_x = basis_table(count_x).reshape(north, share_x, count_x)
    high_y, low_y = np_split(basis_table(count_y))
    high_z, low_z = np_split(basis_table(count_z))
    values = jnp.transpose(velocity, (0, 2, 3, 1))
    part_x = lax.dynamic_slice_in_dim(symbol_x, lax.axis_index("north") * share_x, share_x)
    part_y = lax.dynamic_slice_in_dim(symbol_y, lax.axis_index("deep") * share_y, share_y)
    weight = 1.0 / (1.0 + (part_x[:, None, None] + part_y[None, :, None] + symbol_z))
    out = None
    for first, share in chunks_of(share_x):
        high, low = np_split(table_x[:, first : first + share].reshape(north * share, count_x))
        sent = pl.pallas_call(
            x_kernel,
            out_shape=jax.ShapeDtypeStruct((north, lanes // width, share * lines, width), jnp.float32),
            in_specs=[VMEM] * 3,
            out_specs=VMEM,
            compiler_params=pltpu.CompilerParams(vmem_limit_bytes=16 * 2**20),
            cost_estimate=cost(6 * north * share * count_x * lines * lanes, 4 * values.size),
            name="x_modes",
        )(values, high, low)
        lines_here = lax.all_to_all(sent, "north", split_axis=0, concat_axis=0, tiled=True)
        sent = pl.pallas_call(
            y_kernel,
            out_shape=jax.ShapeDtypeStruct((deep, share, share_y, lanes), jnp.float32),
            in_specs=[VMEM] * 3,
            out_specs=VMEM,
            compiler_params=pltpu.CompilerParams(vmem_limit_bytes=16 * 2**20),
            cost_estimate=cost(6 * count_y * count_y * share * lanes, 8 * sent.size),
            name="y_modes",
        )(lines_here, high_y, low_y)
        lines_here = lax.all_to_all(sent, "deep", split_axis=0, concat_axis=0, tiled=True)
        operands = [lines_here, high_z, low_z, weight[first : first + share], coupling]
        specs = [VMEM] * 4 + [pl.BlockSpec(memory_space=pltpu.SMEM)]
        aliases = {}
        if out is not None:
            operands.append(out)
            specs.append(pl.BlockSpec(memory_space=pl.ANY))
            aliases = {5: 0}
        out = pl.pallas_call(
            functools.partial(z_kernel, first),
            out_shape=jax.ShapeDtypeStruct((fields, share_x, share_y, count_z), jnp.float32),
            in_specs=specs,
            out_specs=pl.BlockSpec(memory_space=pl.ANY),
            scratch_shapes=[
                pltpu.VMEM((fields, share, share_y, count_z), jnp.float32),
                pltpu.SemaphoreType.DMA((fields,)),
            ],
            input_output_aliases=aliases,
            compiler_params=pltpu.CompilerParams(vmem_limit_bytes=16 * 2**20),
            cost_estimate=cost(6 * sent.size * count_z, 8 * sent.size),
            name="z_modes",
        )(*operands)
    return out


def solution(mesh):
    placed = (P(None, None, "north", "deep"), P(), P(), P(), P())
    return jax.shard_map(
        functools.partial(on_device, mesh.shape["north"], mesh.shape["deep"]),
        mesh=mesh,
        in_specs=placed,
        out_specs=P(None, "north", "deep", None),
        check_vma=False,
    )
```
